32 devices in a mesh: pts: 4 (over y, x), med: 8 (over z, core).
Axes of the slice: x: 2, y: 2, z: 4, core: 2. Of those that a mesh axis runs over, the one named last changes fastest.
Arguments:
- points: float32 [65536, 1024], P(('pts', 'med')), may hold values from -6 to 6
- weights: float32 [65536], P(('pts', 'med')), may hold values from 0.2 to 6
- medoid_ids: int32 [512], replicated, may hold values from 0 to 65535, as said below
Outputs:
- cover: float32 [65536], P(('pts', 'med'))
- total: float32 [], replicated
The draws below stay inside these ranges and needn't reach their ends.
Inputs may be any that keep to these rules, and one draw needn't show every extreme that they name: `medoid_ids`: distinct row numbers; the points of one device hold at most 24 medoids, and some device holds exactly 24 in every draw.
All inputs are finite; a program needn't handle non-finite values.
Results may differ from the reference program's by a relative error of at most 0.00005.
Values sent between devices are 32-bit elements; how exact they have to be, the bound alone decides.
A program may use at most 128 MiB of HBM per device.

```python
import jax
import jax.numpy as jnp
from jax import lax

D = 1024
ROWS_DEV = 2048
CAP = 24
POINTS = 65536
MEDOIDS = 512
N_PTS = 4
N_MED = 8


def draw_medoid_ids(key, part):
    devcount = N_PTS * N_MED
    slots = devcount * CAP
    key_rank = jax.random.fold_in(key, 31)
    key_forced = jax.random.fold_in(key, 32)
    key_rows = jax.random.fold_in(key, 33)
    key_order = jax.random.fold_in(key, 34)
    forced = jax.random.randint(key_forced, (), 0, devcount)
    rank = jax.random.permutation(key_rank, slots).astype(jnp.int32)
    owner = jnp.arange(slots, dtype=jnp.int32) // CAP
    rank = jnp.where(owner == forced, rank - slots, rank)
    order = jnp.argsort(rank, stable=True)[:MEDOIDS]
    row_keys = jax.random.split(key_rows, devcount)
    chosen = jax.vmap(lambda kk: jax.random.permutation(kk, ROWS_DEV))(row_keys)[:, :CAP]
    candid = jnp.arange(devcount, dtype=jnp.int32)[:, None] * ROWS_DEV + chosen.astype(jnp.int32)
    picked = candid.reshape(-1)[order]
    return picked[jax.random.permutation(key_order, MEDOIDS)].astype(jnp.int32)


def draw_weights(key, part):
    position = jnp.arange(POINTS, dtype=jnp.float32) / jnp.float32(max(POINTS - 1, 1))
    base = jnp.exp(jax.random.uniform(jax.random.fold_in(key, 22), (POINTS,), jnp.float32, -0.69, 0.69))
    ramp = 1.0 + 2.0 * position
    return (base * ramp).astype(jnp.float32)


def steps_of(own_key, extent, pieces, low, top_value):
    def one(dim, shards_of):
        steps = jax.random.uniform(jax.random.fold_in(jax.random.fold_in(own_key, 6), dim), (shards_of,), jnp.float32, low / len(pieces), top_value / len(pieces))
        return jnp.repeat(jnp.exp(steps), extent[dim] // shards_of).reshape((-1,) + (1,) * (len(extent) - dim - 1))

    factor_of = one(*pieces[0])
    for cut in pieces[1:]:
        factor_of = factor_of * one(*cut)
    return factor_of


def scatter_about(stream_key, shape, deviation, reach, pieces=(), kind=jnp.bfloat16):
    drawn = jax.random.normal(stream_key, shape, jnp.float32) * deviation
    if len(pieces) > 0:
        drawn = steps_of(stream_key, shape, pieces, -0.22, 0.18) * drawn
    return jnp.clip(drawn, min=-reach, max=reach).astype(kind)


def setup_inputs(seed: int = 0) -> dict:
    key_of = jax.random.split(jax.random.key(seed), 4)
    return {
        "points": scatter_about(key_of[0], (POINTS, D), 1.0, 6.0, ((0, 32),), jnp.float32),
        "weights": draw_weights(jax.random.fold_in(key_of[3], 71), 0),
        "medoid_ids": draw_medoid_ids(jax.random.fold_in(key_of[3], 71), 0),
    }


EPS = 1e-06

def reference(points, weights, medoid_ids):
    unit = points * lax.rsqrt(lax.optimization_barrier(jnp.sum(points * points, axis=1, keepdims=True)) + EPS)
    centers = jnp.take(unit, medoid_ids.astype(jnp.int32), axis=0)
    blocks = unit.reshape(POINTS // ROWS_DEV, ROWS_DEV, D)

    def block_cover(rows):
        sims = lax.dot_general(rows, centers, (((1,), (1,)), ((), ())), precision=lax.Precision.HIGHEST, preferred_element_type=jnp.float32)
        return lax.optimization_barrier(jnp.max(sims, axis=1))
    cover = lax.map(block_cover, blocks).reshape(POINTS)
    total = jnp.sum(weights * cover) / jnp.sum(weights)
    return (cover, total)
```

```python
import functools

import jax
import jax.numpy as jnp
from jax import lax
from jax.experimental import pallas as pl
from jax.experimental.pallas import tpu as pltpu
from jax.sharding import PartitionSpec as P

MED_DEV = 16
CAPACITY = MED_DEV + MED_DEV // 2
EPS = 1e-06
CORES = 2
TILE = 256


def gather_kernel(start_ref, ids_ref, points_ref, out_ref, pos_ref, buf_ref, sem):
    rows = points_ref.shape[0]
    start = start_ref[0]
    for slot in range(CAPACITY):
        pos_ref[slot] = 0

    def scan(step, count):
        for lane in range(8):
            local = ids_ref[step * 8 + lane] - start
            owned = jnp.logical_and(local >= 0, local < rows)
            pos_ref[count] = jnp.where(owned, local, 0)
            count = count + owned.astype(jnp.int32)
        return count

    lax.fori_loop(0, ids_ref.shape[0] // 8, scan, jnp.int32(0))

    def row_copy(slot):
        return pltpu.make_async_copy(
            points_ref.at[pl.ds(pos_ref[slot], 1)], buf_ref.at[pl.ds(slot, 1)], sem.at[slot]
        )

    for slot in range(CAPACITY):
        row_copy(slot).start()
    for slot in range(CAPACITY):
        row_copy(slot).wait()
    block = buf_ref[...]
    out_ref[...] = block * lax.rsqrt(jnp.sum(block * block, axis=1, keepdims=True) + EPS)


def split(value):
    high = value.astype(jnp.bfloat16)
    return high, (value - high.astype(jnp.float32)).astype(jnp.bfloat16)


def cover_kernel(
    group_pts, group_med, mine_ref, points_ref, weights_ref, ids_ref, cover_ref, total_ref,
    recv, pbuf, phigh, plow, chigh, clow, offs, best, scale, part, tin,
    psem, msem, rsem, zsem, fsem, ssem, bsem, tsend, trecv,
):
    rows = points_ref.shape[0]
    tiles = rows // TILE
    n_z = group_med // CORES
    n_a = 2
    n_b = group_pts // n_a
    swap = n_a == n_b
    n_1, n_2 = n_b, n_a
    me_pts = lax.axis_index("pts")
    me_med = lax.axis_index("med")
    core = lax.rem(me_med, CORES)
    zed = me_med // CORES
    a, b = me_pts // n_b, lax.rem(me_pts, n_b)
    other = 1 - core

    def axes_of(which):
        if swap:
            return jnp.where(which == 0, b, a), jnp.where(which == 0, a, b)
        return b, a

    def pts_of(which, i_1, i_2):
        if swap:
            return jnp.where(which == 0, i_2 * n_b + i_1, i_1 * n_b + i_2)
        return i_2 * n_b + i_1

    i_1, i_2 = axes_of(core)
    o_1, o_2 = axes_of(other)

    def dev_z(step):
        return {"pts": me_pts, "med": lax.rem(zed + step, n_z) * CORES + core}

    def dev_1(step):
        return {"pts": pts_of(core, lax.rem(i_1 + step, n_1), i_2), "med": me_med}

    def dev_2(step):
        return {"pts": pts_of(core, i_1, lax.rem(i_2 + step, n_2)), "med": me_med}

    sibling = {"pts": me_pts, "med": zed * CORES + other}
    partners = (
        [dev_z(step) for step in range(1, n_z)]
        + [dev_1(step) for step in range(1, n_1)]
        + [dev_2(step) for step in range(1, n_2)]
        + [sibling]
    )

    def points_copy(tile):
        part_of = pl.ds(pl.multiple_of(tile * TILE, TILE), TILE)
        return pltpu.make_async_copy(points_ref.at[part_of], pbuf.at[part_of], psem.at[tile])

    own_copy = pltpu.make_async_copy(mine_ref, recv.at[core, i_2, i_1, zed], msem)
    own_copy.start()
    for tile in range(tiles):
        points_copy(tile).start()
    barrier = pltpu.get_barrier_semaphore()
    for partner in partners:
        pl.semaphore_signal(barrier, inc=1, device_id=partner, device_id_type=pl.DeviceIdType.MESH)
    pl.semaphore_wait(barrier, len(partners))

    def send(src, j_2, j_1, z, sem, partner):
        return pltpu.make_async_remote_copy(
            src_ref=src,
            dst_ref=recv.at[core, j_2, j_1, z],
            send_sem=sem,
            recv_sem=rsem.at[core, j_2, j_1, z],
            device_id=partner,
            device_id_type=pl.DeviceIdType.MESH,
        )

    def send_z(step):
        return send(mine_ref, i_2, i_1, zed, zsem.at[step], dev_z(step))

    def send_1(z, step, src=None):
        src = recv.at[core, i_2, i_1, z] if src is None else src
        return send(src, i_2, i_1, z, fsem.at[z, step], dev_1(step))

    def send_2(j_1, z, step, src=None):
        src = recv.at[core, i_2, j_1, z] if src is None else src
        return send(src, i_2, j_1, z, ssem.at[j_1, z, step], dev_2(step))

    def send_b(j_2, j_1, z, src=None):
        src = recv.at[core, j_2, j_1, z] if src is None else src
        return send(src, j_2, j_1, z, bsem.at[j_2, j_1, z], sibling)

    def arrived(which, j_2, j_1, z):
        slot = recv.at[which, j_2, j_1, z]
        pltpu.make_async_copy(slot, slot, rsem.at[which, j_2, j_1, z]).wait()

    def z_at(step):
        return lax.rem(zed + step, n_z)

    def one_at(step):
        return lax.rem(i_1 + step, n_1)

    def two_at(step):
        return lax.rem(i_2 + step, n_2)

    for step in range(1, n_1):
        send_1(zed, step, mine_ref).start()
    for step in range(1, n_2):
        send_2(i_1, zed, step, mine_ref).start()
    for step in [1, n_z - 1] + list(range(2, n_z - 1)) if n_z > 2 else range(1, n_z):
        send_z(step).start()
    send_b(i_2, i_1, zed, mine_ref).start()

    best[...] = jnp.full(best.shape, -1e30, jnp.float32)

    def prepare(tile, carry):
        points_copy(tile).wait()
        part_of = pl.ds(pl.multiple_of(tile * TILE, TILE), TILE)
        value = pbuf[part_of, :]
        high, low = split(value)
        phigh[part_of, :] = high
        plow[part_of, :] = low
        square = value * value
        lanes = square[:, :128]
        for k in range(1, square.shape[1] // 128):
            lanes = lanes + square[:, k * 128 : (k + 1) * 128]
        norm = jnp.sum(lanes.T, axis=0, keepdims=True)
        scale[:, part_of] = jnp.broadcast_to(lax.rsqrt(norm + EPS), (8, TILE))
        return carry

    lax.fori_loop(0, tiles, prepare, 0)
    own_copy.wait()

    z_order = [1, n_z - 1] + list(range(2, n_z - 1)) if n_z > 2 else list(range(1, n_z))
    for step in z_order:
        z = z_at(step)
        arrived(core, i_2, i_1, z)
        for hop in range(1, n_1):
            send_1(z, hop).start()
        for hop in range(1, n_2):
            send_2(i_1, z, hop).start()
        send_b(i_2, i_1, z).start()

    width = n_z * CAPACITY
    ids = ids_ref[...]

    def load_chunk(which, j_2, j_1, base):
        value = recv[which, j_2, j_1].reshape(width, recv.shape[-1])
        high, low = split(value)
        chigh[base : base + width, :] = high
        clow[base : base + width, :] = low
        at = lax.broadcasted_iota(jnp.int32, (width, 1), 0)
        z = at // CAPACITY
        slot = at - z * CAPACITY
        first = (pts_of(which, j_1, j_2) * group_med + z * CORES + which) * rows
        inside = jnp.logical_and(ids >= first, ids < first + rows)
        count = jnp.sum(jnp.where(inside, 1.0, 0.0), axis=1, keepdims=True)
        offs[base : base + width, :] = jnp.where(slot.astype(jnp.float32) < count, 0.0, -1e30)

    dims = (((1,), (1,)), ((), ()))

    def multiply(tile):
        part_of = pl.ds(pl.multiple_of(tile * TILE, TILE), TILE)
        dot = functools.partial(lax.dot_general, dimension_numbers=dims, preferred_element_type=jnp.float32)
        high, low = phigh[part_of, :], plow[part_of, :]
        sims = dot(clow[...], high) + dot(chigh[...], low) + dot(chigh[...], high)
        sims = sims + offs[...]
        top = jnp.max(sims.reshape(-1, 8, TILE), axis=0)
        best[:, part_of] = jnp.maximum(best[:, part_of], top)

    def event_1(e):
        hop = e // n_z + 1
        z = z_at(lax.rem(e, n_z))
        j_1 = one_at(hop)
        arrived(core, i_2, j_1, z)
        for far in range(1, n_2):
            send_2(j_1, z, far).start()
        send_b(i_2, j_1, z).start()

    def event_2(one, e):
        hop = e // n_z + 1
        z = z_at(lax.rem(e, n_z))
        j_2 = two_at(hop)
        arrived(core, j_2, one_at(one), z)
        send_b(j_2, one_at(one), z).start()

    def chunk(e_2, e_1, event, events):
        for z in range(n_z):
            if swap:
                s_2, s_1 = lax.rem(o_2 + e_2, n_2), lax.rem(o_1 + e_1, n_1)
            else:
                s_2, s_1 = two_at(e_2), one_at(e_1)
            if not (e_2 == 0 and e_1 == 0):
                pass
            arrived(other, s_2, s_1, z)
        load_chunk(core, two_at(e_2), one_at(e_1), 0)
        load_chunk(other, s_2, s_1, width)

        def step(tile, carry):
            if events:
                @pl.when(tile < events)
                def _():
                    event(tile)
            multiply(tile)
            return carry

        lax.fori_loop(0, tiles, step, 0)
        if events > tiles:
            def rest(e, carry):
                event(e)
                return carry

            lax.fori_loop(tiles, events, rest, 0)

    order = [(e_2, e_1) for e_2 in range(n_2) for e_1 in range(n_1)]
    for e_2, e_1 in order:
        if e_2 == 0 and e_1 == 0:
            chunk(0, 0, event_1, (n_1 - 1) * n_z)
        elif e_2 == 0:
            last = e_1 == n_1 - 1
            if last:
                chunk(0, e_1, functools.partial(event_2, 0), (n_2 - 1) * n_z)
            else:
                chunk(0, e_1, None, 0)
        elif e_2 == 1:
            if e_1 + 1 < n_1:
                chunk(1, e_1, functools.partial(event_2, e_1 + 1), (n_2 - 1) * n_z)
            else:
                chunk(1, e_1, None, 0)
        else:
            chunk(e_2, e_1, None, 0)

    cover = jnp.max(best[...], axis=0, keepdims=True) * scale[0:1, :]
    cover_ref[...] = cover
    weights = weights_ref[...]
    lane = lax.broadcasted_iota(jnp.int32, (8, 128), 1)
    number = jnp.sum(weights * cover, axis=1, keepdims=True)
    weight = jnp.sum(weights, axis=1, keepdims=True)
    value = jnp.where(lane == 0, number, weight)

    stages = [
        (n_z, zed, dev_z), (n_1, i_1, dev_1), (n_2, i_2, dev_2), (CORES, core, lambda step: sibling),
    ]
    copies = []
    for stage, (extent, index, partner_of) in enumerate(stages):
        if extent == 1:
            continue
        part[stage] = value
        for step in range(1, extent):
            copy = pltpu.make_async_remote_copy(
                src_ref=part.at[stage],
                dst_ref=tin.at[stage, index],
                send_sem=tsend.at[stage, step],
                recv_sem=trecv.at[stage, index],
                device_id=partner_of(step),
                device_id_type=pl.DeviceIdType.MESH,
            )
            copy.start()
            copies.append(copy)
        for step in range(1, extent):
            where = lax.rem(index + step, extent)
            slot = tin.at[stage, where]
            pltpu.make_async_copy(slot, slot, trecv.at[stage, where]).wait()
        tin[stage, index] = value
        value = tin[stage, 0]
        for at in range(1, extent):
            value = value + tin[stage, at]
    total_ref[...] = value[:, 0:1] / value[:, 1:2] + jnp.zeros((8, 128), jnp.float32)

    for step in range(1, n_z):
        send_z(step).wait_send()
    for z in range(n_z):
        for step in range(1, n_1):
            send_1(z, step).wait_send()
        for j_1 in range(n_1):
            for step in range(1, n_2):
                send_2(j_1, z, step).wait_send()
            for j_2 in range(n_2):
                send_b(j_2, j_1, z).wait_send()
    for copy in copies:
        copy.wait_send()


def body(points, weights, medoid_ids):
    rows, width = points.shape
    group_pts = lax.axis_size("pts")
    group_med = lax.axis_size("med")
    n_z, n_a = group_med // CORES, 2
    n_1, n_2 = group_pts // n_a, n_a
    start = (lax.axis_index("pts") * group_med + lax.axis_index("med")) * rows
    smem = pl.BlockSpec(memory_space=pltpu.SMEM)
    vmem = pl.BlockSpec(memory_space=pltpu.VMEM)
    hbm = pl.BlockSpec(memory_space=pl.ANY)
    mine = pl.pallas_call(
        gather_kernel,
        out_shape=jax.ShapeDtypeStruct((CAPACITY, width), jnp.float32),
        in_specs=[smem, smem, hbm],
        out_specs=vmem,
        scratch_shapes=[
            pltpu.SMEM((CAPACITY + 1,), jnp.int32),
            pltpu.VMEM((CAPACITY, width), jnp.float32),
            pltpu.SemaphoreType.DMA((CAPACITY,)),
        ],
        name="gather_rows",
    )(start[None].astype(jnp.int32), medoid_ids, points)

    chunk = CORES * n_z * CAPACITY
    top = max(n_z, n_1, n_2, CORES)
    dma = pltpu.SemaphoreType.DMA
    cover, total = pl.pallas_call(
        functools.partial(cover_kernel, group_pts, group_med),
        out_shape=[
            jax.ShapeDtypeStruct((1, rows), jnp.float32),
            jax.ShapeDtypeStruct((8, 128), jnp.float32),
        ],
        in_specs=[vmem, hbm, vmem, vmem],
        out_specs=[vmem, vmem],
        scratch_shapes=[
            pltpu.VMEM((CORES, n_2, n_1, n_z, CAPACITY, width), jnp.float32),
            pltpu.VMEM((rows, width), jnp.float32),
            pltpu.VMEM((rows, width), jnp.bfloat16),
            pltpu.VMEM((rows, width), jnp.bfloat16),
            pltpu.VMEM((chunk, width), jnp.bfloat16),
            pltpu.VMEM((chunk, width), jnp.bfloat16),
            pltpu.VMEM((chunk, 1), jnp.float32),
            pltpu.VMEM((8, rows), jnp.float32),
            pltpu.VMEM((8, rows), jnp.float32),
            pltpu.VMEM((4, 8, 128), jnp.float32),
            pltpu.VMEM((4, top, 8, 128), jnp.float32),
            dma((rows // TILE,)),
            dma,
            dma((CORES, n_2, n_1, n_z)),
            dma((n_z,)),
            dma((n_z, n_1)),
            dma((n_1, n_z, n_2)),
            dma((n_2, n_1, n_z)),
            dma((4, top)),
            dma((4, top)),
        ],
        compiler_params=pltpu.CompilerParams(
            collective_id=0, has_side_effects=True, vmem_limit_bytes=60 * 1024 * 1024
        ),
        name="cover_all",
    )(mine, points, weights[None, :], medoid_ids[None, :])
    return cover.reshape(rows), total[0, 0]


def solution(mesh):
    return jax.shard_map(
        body,
        mesh=mesh,
        in_specs=(P(("pts", "med"), None), P(("pts", "med")), P()),
        out_specs=(P(("pts", "med")), P()),
        check_vma=False,
    )
```

```python
import functools

import jax
import jax.numpy as jnp
from jax import lax
from jax.experimental import pallas as pl
from jax.experimental.pallas import tpu as pltpu
from jax.sharding import PartitionSpec as P

MED_DEV = 16
CAPACITY = MED_DEV + MED_DEV // 2
EPS = 1e-06
CORES = 2
TILE = 256
PIECE = 32


def gather_kernel(start_ref, ids_ref, points_ref, out_ref, pos_ref, buf_ref, sem):
    rows = points_ref.shape[0]
    start = start_ref[0]
    for slot in range(CAPACITY):
        pos_ref[slot] = 0

    def scan(step, count):
        for lane in range(8):
            local = ids_ref[step * 8 + lane] - start
            owned = jnp.logical_and(local >= 0, local < rows)
            pos_ref[count] = jnp.where(owned, local, 0)
            count = count + owned.astype(jnp.int32)
        return count

    lax.fori_loop(0, ids_ref.shape[0] // 8, scan, jnp.int32(0))

    def row_copy(slot):
        return pltpu.make_async_copy(
            points_ref.at[pl.ds(pos_ref[slot], 1)], buf_ref.at[pl.ds(slot, 1)], sem.at[slot]
        )

    for slot in range(CAPACITY):
        row_copy(slot).start()
    for slot in range(CAPACITY):
        row_copy(slot).wait()
    block = buf_ref[...]
    out_ref[...] = block * lax.rsqrt(jnp.sum(block * block, axis=1, keepdims=True) + EPS)


def split(value):
    high = value.astype(jnp.bfloat16)
    return high, (value - high.astype(jnp.float32)).astype(jnp.bfloat16)


def cover_kernel(
    group_pts, group_med, mine_ref, points_ref, weights_ref, ids_ref, cover_ref, total_ref,
    recv, pbuf, pcat, ccat, offs, lanes, best, part, tin,
    psem, msem, rsem, zsem, fsem, ssem, bsem, tsend, trecv,
):
    rows = points_ref.shape[0]
    tiles = rows // TILE
    n_z = group_med // CORES
    n_a = 2
    n_b = group_pts // n_a
    swap = n_a == n_b
    n_1, n_2 = n_b, n_a
    me_pts = lax.axis_index("pts")
    me_med = lax.axis_index("med")
    core = lax.rem(me_med, CORES)
    zed = me_med // CORES
    a, b = me_pts // n_b, lax.rem(me_pts, n_b)
    other = 1 - core

    def axes_of(which):
        if swap:
            return jnp.where(which == 0, b, a), jnp.where(which == 0, a, b)
        return b, a

    def pts_of(which, i_1, i_2):
        if swap:
            return jnp.where(which == 0, i_2 * n_b + i_1, i_1 * n_b + i_2)
        return i_2 * n_b + i_1

    i_1, i_2 = axes_of(core)
    o_1, o_2 = axes_of(other)

    def dev_z(step):
        return {"pts": me_pts, "med": lax.rem(zed + step, n_z) * CORES + core}

    def dev_1(step):
        return {"pts": pts_of(core, lax.rem(i_1 + step, n_1), i_2), "med": me_med}

    def dev_2(step):
        return {"pts": pts_of(core, i_1, lax.rem(i_2 + step, n_2)), "med": me_med}

    sibling = {"pts": me_pts, "med": zed * CORES + other}
    plane = group_pts * CORES
    place = me_pts * CORES + core

    def dev_plane(step):
        at = lax.rem(place + step, plane)
        return {"pts": at // CORES, "med": zed * CORES + lax.rem(at, CORES)}

    partners = [dev_z(step) for step in range(1, n_z)] + [dev_plane(step) for step in range(1, plane)]

    def points_copy(tile):
        part_of = pl.ds(pl.multiple_of(tile * TILE, TILE), TILE)
        return pltpu.make_async_copy(points_ref.at[part_of], pbuf.at[part_of], psem.at[tile])

    own_copy = pltpu.make_async_copy(mine_ref, recv.at[core, i_2, i_1, zed], msem)
    own_copy.start()
    for tile in range(tiles):
        points_copy(tile).start()
    barrier = pltpu.get_barrier_semaphore()
    for partner in partners:
        pl.semaphore_signal(barrier, inc=1, device_id=partner, device_id_type=pl.DeviceIdType.MESH)

    width = n_z * CAPACITY
    depth = points_ref.shape[1]
    ids = ids_ref[...]

    def offsets(which, j_2, j_1):
        at = lax.broadcasted_iota(jnp.int32, (width, 1), 0)
        z = at // CAPACITY
        slot = at - z * CAPACITY
        first = (pts_of(which, j_1, j_2) * group_med + z * CORES + which) * rows
        inside = jnp.logical_and(ids >= first, ids < first + rows)
        count = jnp.sum(jnp.where(inside, 1.0, 0.0), axis=1, keepdims=True)
        offs[which, j_2, j_1] = jnp.where(slot.astype(jnp.float32) < count, 0.0, -1e30)

    def offsets_at(at, carry):
        which = at // (n_1 * n_2)
        j_2 = lax.rem(at, n_1 * n_2) // n_1
        offsets(which, j_2, lax.rem(at, n_1))
        return carry

    lax.fori_loop(0, CORES * n_1 * n_2, offsets_at, 0)
    best[...] = jnp.full(best.shape, -1e30, jnp.float32)
    pl.semaphore_wait(barrier, len(partners))

    def send(src, j_2, j_1, z, sem, partner):
        return pltpu.make_async_remote_copy(
            src_ref=src,
            dst_ref=recv.at[core, j_2, j_1, z],
            send_sem=sem,
            recv_sem=rsem.at[core, j_2, j_1, z],
            device_id=partner,
            device_id_type=pl.DeviceIdType.MESH,
        )

    def send_z(step):
        return send(mine_ref, i_2, i_1, zed, zsem.at[step], dev_z(step))

    def send_1(z, step, src=None):
        src = recv.at[core, i_2, i_1, z] if src is None else src
        return send(src, i_2, i_1, z, fsem.at[z, step], dev_1(step))

    def send_2(j_1, z, step, src=None):
        src = recv.at[core, i_2, j_1, z] if src is None else src
        return send(src, i_2, j_1, z, ssem.at[j_1, z, step], dev_2(step))

    def send_b(j_2, j_1, z, src=None):
        src = recv.at[core, j_2, j_1, z] if src is None else src
        return send(src, j_2, j_1, z, bsem.at[j_2, j_1, z], sibling)

    def arrived(which, j_2, j_1, z):
        slot = recv.at[which, j_2, j_1, z]
        pltpu.make_async_copy(slot, slot, rsem.at[which, j_2, j_1, z]).wait()

    def z_at(step):
        return lax.rem(zed + step, n_z)

    def one_at(step):
        return lax.rem(i_1 + step, n_1)

    def two_at(step):
        return lax.rem(i_2 + step, n_2)

    for step in range(1, n_1):
        send_1(zed, step, mine_ref).start()
    for step in range(1, n_2):
        send_2(i_1, zed, step, mine_ref).start()
    for step in [1, n_z - 1] + list(range(2, n_z - 1)) if n_z > 2 else range(1, n_z):
        send_z(step).start()
    send_b(i_2, i_1, zed, mine_ref).start()

    def prepare(tile, carry):
        points_copy(tile).wait()

        def piece(step, carry):
            part_of = pl.ds(pl.multiple_of(tile * TILE + step * PIECE, PIECE), PIECE)
            value = pbuf[part_of, :]
            high, low = split(value)
            pcat[part_of, 0:depth] = high
            pcat[part_of, depth : 2 * depth] = low
            pcat[part_of, 2 * depth : 3 * depth] = high
            square = value * value
            total = square[:, :128]
            for k in range(1, depth // 128):
                total = total + square[:, k * 128 : (k + 1) * 128]
            lanes[part_of, :] = total
            return carry

        lax.fori_loop(0, TILE // PIECE, piece, 0)
        return carry

    lax.fori_loop(0, tiles, prepare, 0)
    own_copy.wait()

    z_order = [1, n_z - 1] + list(range(2, n_z - 1)) if n_z > 2 else list(range(1, n_z))
    for step in z_order:
        z = z_at(step)
        arrived(core, i_2, i_1, z)
        for hop in range(1, n_1):
            send_1(z, hop).start()
        for hop in range(1, n_2):
            send_2(i_1, z, hop).start()
        send_b(i_2, i_1, z).start()

    def load_chunk(which, j_2, j_1, base):
        def pair(step, carry):
            value = recv[which, j_2, j_1, pl.ds(step * 2, 2)].reshape(2 * CAPACITY, depth)
            high, low = split(value)
            part_of = pl.ds(pl.multiple_of(base + step * 2 * CAPACITY, 2 * CAPACITY), 2 * CAPACITY)
            ccat[part_of, 0:depth] = high
            ccat[part_of, depth : 2 * depth] = high
            ccat[part_of, 2 * depth : 3 * depth] = low
            return carry

        lax.fori_loop(0, n_z // 2, pair, 0)

    dims = (((1,), (1,)), ((), ()))

    def multiply(tile, mask):
        part_of = pl.ds(pl.multiple_of(tile * TILE, TILE), TILE)
        sims = lax.dot_general(ccat[...], pcat[part_of, :], dims, preferred_element_type=jnp.float32)
        sims = sims + mask()
        top = jnp.max(sims.reshape(-1, 8, TILE), axis=0)
        best[:, part_of] = jnp.maximum(best[:, part_of], top)

    def event_1(e):
        hop = e // n_z + 1
        z = z_at(lax.rem(e, n_z))
        j_1 = one_at(hop)
        arrived(core, i_2, j_1, z)
        for far in range(1, n_2):
            send_2(j_1, z, far).start()
        send_b(i_2, j_1, z).start()

    def event_2(one, e):
        hop = e // n_z + 1
        z = z_at(lax.rem(e, n_z))
        j_2 = two_at(hop)
        arrived(core, j_2, one_at(one), z)
        send_b(j_2, one_at(one), z).start()

    def chunk(e_2, e_1, event, events):
        for z in range(n_z):
            if swap:
                s_2, s_1 = lax.rem(o_2 + e_2, n_2), lax.rem(o_1 + e_1, n_1)
            else:
                s_2, s_1 = two_at(e_2), one_at(e_1)
            arrived(other, s_2, s_1, z)
        load_chunk(core, two_at(e_2), one_at(e_1), 0)
        load_chunk(other, s_2, s_1, width)

        def mask():
            return jnp.concatenate(
                [offs[core, two_at(e_2), one_at(e_1)], offs[other, s_2, s_1]], axis=0
            )

        def step(tile, carry):
            if events:
                @pl.when(tile < events)
                def _():
                    event(tile)
            multiply(tile, mask)
            return carry

        lax.fori_loop(0, tiles, step, 0)
        if events > tiles:
            def rest(e, carry):
                event(e)
                return carry

            lax.fori_loop(tiles, events, rest, 0)

    norms = [
        jnp.sum(lanes[k * 128 : (k + 1) * 128, :].T, axis=0, keepdims=True) for k in range(rows // 128)
    ]
    scale = lax.rsqrt(jnp.concatenate(norms, axis=1) + EPS)

    order = [(e_2, e_1) for e_2 in range(n_2) for e_1 in range(n_1)]
    for e_2, e_1 in order:
        if e_2 == 0 and e_1 == 0:
            chunk(0, 0, event_1, (n_1 - 1) * n_z)
        elif e_2 == 0:
            last = e_1 == n_1 - 1
            if last:
                chunk(0, e_1, functools.partial(event_2, 0), (n_2 - 1) * n_z)
            else:
                chunk(0, e_1, None, 0)
        elif e_2 == 1:
            if e_1 + 1 < n_1:
                chunk(1, e_1, functools.partial(event_2, e_1 + 1), (n_2 - 1) * n_z)
            else:
                chunk(1, e_1, None, 0)
        else:
            chunk(e_2, e_1, None, 0)

    cover = jnp.max(best[...], axis=0, keepdims=True) * scale
    cover_ref[...] = cover
    weights = weights_ref[...]
    lane = lax.broadcasted_iota(jnp.int32, (8, 128), 1)
    number = jnp.sum(weights * cover, axis=1, keepdims=True)
    weight = jnp.sum(weights, axis=1, keepdims=True)
    value = jnp.where(lane == 0, number, weight)

    stages = [(n_z, zed, dev_z), (plane, place, dev_plane)]
    copies = []
    for stage, (extent, index, partner_of) in enumerate(stages):
        if extent == 1:
            continue
        part[stage] = value
        for step in range(1, extent):
            copy = pltpu.make_async_remote_copy(
                src_ref=part.at[stage],
                dst_ref=tin.at[stage, index],
                send_sem=tsend.at[stage, step],
                recv_sem=trecv.at[stage, index],
                device_id=partner_of(step),
                device_id_type=pl.DeviceIdType.MESH,
            )
            copy.start()
            copies.append(copy)
        for step in range(1, extent):
            where = lax.rem(index + step, extent)
            slot = tin.at[stage, where]
            pltpu.make_async_copy(slot, slot, trecv.at[stage, where]).wait()
        tin[stage, index] = value
        value = tin[stage, 0]
        for at in range(1, extent):
            value = value + tin[stage, at]
    total_ref[...] = value[:, 0:1] / value[:, 1:2] + jnp.zeros((8, 128), jnp.float32)

    for step in range(1, n_z):
        send_z(step).wait_send()
    for z in range(n_z):
        for step in range(1, n_1):
            send_1(z, step).wait_send()
        for j_1 in range(n_1):
            for step in range(1, n_2):
                send_2(j_1, z, step).wait_send()
            for j_2 in range(n_2):
                send_b(j_2, j_1, z).wait_send()
    for copy in copies:
        copy.wait_send()


def finish_kernel(cover_ref, total_ref, out_ref, mean_ref):
    out_ref[...] = cover_ref[...]
    mean_ref[0, 0] = total_ref[0, 0]


def body(points, weights, medoid_ids):
    rows, width = points.shape
    group_pts = lax.axis_size("pts")
    group_med = lax.axis_size("med")
    n_z, n_a = group_med // CORES, 2
    n_1, n_2 = group_pts // n_a, n_a
    start = (lax.axis_index("pts") * group_med + lax.axis_index("med")) * rows
    smem = pl.BlockSpec(memory_space=pltpu.SMEM)
    vmem = pl.BlockSpec(memory_space=pltpu.VMEM)
    hbm = pl.BlockSpec(memory_space=pl.ANY)
    mine = pl.pallas_call(
        gather_kernel,
        out_shape=jax.ShapeDtypeStruct((CAPACITY, width), jnp.float32),
        in_specs=[smem, smem, hbm],
        out_specs=vmem,
        scratch_shapes=[
            pltpu.SMEM((CAPACITY + 1,), jnp.int32),
            pltpu.VMEM((CAPACITY, width), jnp.float32),
            pltpu.SemaphoreType.DMA((CAPACITY,)),
        ],
        name="gather_rows",
    )(start[None].astype(jnp.int32), medoid_ids, points)

    chunk = CORES * n_z * CAPACITY
    top = max(n_z, group_pts * CORES)
    dma = pltpu.SemaphoreType.DMA
    cover, total = pl.pallas_call(
        functools.partial(cover_kernel, group_pts, group_med),
        out_shape=[
            jax.ShapeDtypeStruct((1, rows), jnp.float32),
            jax.ShapeDtypeStruct((8, 128), jnp.float32),
        ],
        in_specs=[vmem, hbm, vmem, vmem],
        out_specs=[vmem, vmem],
        scratch_shapes=[
            pltpu.VMEM((CORES, n_2, n_1, n_z, CAPACITY, width), jnp.float32),
            pltpu.VMEM((rows, width), jnp.float32),
            pltpu.VMEM((rows, 3 * width), jnp.bfloat16),
            pltpu.VMEM((chunk, 3 * width), jnp.bfloat16),
            pltpu.VMEM((CORES, n_2, n_1, n_z * CAPACITY, 1), jnp.float32),
            pltpu.VMEM((rows, 128), jnp.float32),
            pltpu.VMEM((8, rows), jnp.float32),
            pltpu.VMEM((2, 8, 128), jnp.float32),
            pltpu.VMEM((2, top, 8, 128), jnp.float32),
            dma((rows // TILE,)),
            dma,
            dma((CORES, n_2, n_1, n_z)),
            dma((n_z,)),
            dma((n_z, n_1)),
            dma((n_1, n_z, n_2)),
            dma((n_2, n_1, n_z)),
            dma((2, top)),
            dma((2, top)),
        ],
        compiler_params=pltpu.CompilerParams(
            collective_id=0, has_side_effects=True, vmem_limit_bytes=60 * 1024 * 1024
        ),
        name="cover_all",
    )(mine, points, weights[None, :], medoid_ids[None, :])
    cover, total = pl.pallas_call(
        finish_kernel,
        out_shape=[
            jax.ShapeDtypeStruct((1, rows), jnp.float32),
            jax.ShapeDtypeStruct((1, 1), jnp.float32),
        ],
        in_specs=[vmem, vmem],
        out_specs=[vmem, smem],
        name="finish",
    )(cover, total)
    return cover.reshape(rows), total.reshape(())


def solution(mesh):
    return jax.shard_map(
        body,
        mesh=mesh,
        in_specs=(P(("pts", "med"), None), P(("pts", "med")), P()),
        out_specs=(P(("pts", "med")), P()),
        check_vma=False,
    )
```

```python
import functools

import jax
import jax.numpy as jnp
from jax import lax
from jax.experimental import pallas as pl
from jax.experimental.pallas import tpu as pltpu
from jax.sharding import PartitionSpec as P

MED_DEV = 16
CAPACITY = MED_DEV + MED_DEV // 2
EPS = 1e-06
CORES = 2
TILE = 256
PIECE = 128


def gather_kernel(start_ref, ids_ref, points_ref, out_ref, pos_ref, buf_ref, sem):
    rows = points_ref.shape[0]
    start = start_ref[0]
    for slot in range(CAPACITY):
        pos_ref[slot] = 0

    def scan(step, count):
        for lane in range(8):
            local = ids_ref[step * 8 + lane] - start
            owned = jnp.logical_and(local >= 0, local < rows)
            pos_ref[count] = jnp.where(owned, local, 0)
            count = count + owned.astype(jnp.int32)
        return count

    lax.fori_loop(0, ids_ref.shape[0] // 8, scan, jnp.int32(0))

    def row_copy(slot):
        return pltpu.make_async_copy(
            points_ref.at[pl.ds(pos_ref[slot], 1)], buf_ref.at[pl.ds(slot, 1)], sem.at[slot]
        )

    for slot in range(CAPACITY):
        row_copy(slot).start()
    for slot in range(CAPACITY):
        row_copy(slot).wait()
    block = buf_ref[...]
    out_ref[...] = block * lax.rsqrt(jnp.sum(block * block, axis=1, keepdims=True) + EPS)


def split(value):
    high = value.astype(jnp.bfloat16)
    return high, (value - high.astype(jnp.float32)).astype(jnp.bfloat16)


def cover_kernel(
    group_pts, group_med, mine_ref, points_ref, weights_ref, ids_ref, cover_ref, total_ref,
    recv, pbuf, pcat, ccat, offs, scale_ref, best, part, tin,
    psem, msem, rsem, zsem, fsem, ssem, bsem, tsend, trecv,
):
    rows = points_ref.shape[0]
    tiles = rows // TILE
    n_z = group_med // CORES
    n_a = 2
    n_b = group_pts // n_a
    swap = n_a == n_b
    n_1, n_2 = n_b, n_a
    me_pts = lax.axis_index("pts")
    me_med = lax.axis_index("med")
    core = lax.rem(me_med, CORES)
    zed = me_med // CORES
    a, b = me_pts // n_b, lax.rem(me_pts, n_b)
    other = 1 - core

    def axes_of(which):
        if swap:
            return jnp.where(which == 0, b, a), jnp.where(which == 0, a, b)
        return b, a

    def pts_of(which, i_1, i_2):
        if swap:
            return jnp.where(which == 0, i_2 * n_b + i_1, i_1 * n_b + i_2)
        return i_2 * n_b + i_1

    i_1, i_2 = axes_of(core)
    o_1, o_2 = axes_of(other)

    def dev_z(step):
        return {"pts": me_pts, "med": lax.rem(zed + step, n_z) * CORES + core}

    def dev_1(step):
        return {"pts": pts_of(core, lax.rem(i_1 + step, n_1), i_2), "med": me_med}

    def dev_2(step):
        return {"pts": pts_of(core, i_1, lax.rem(i_2 + step, n_2)), "med": me_med}

    sibling = {"pts": me_pts, "med": zed * CORES + other}
    plane = group_pts * CORES
    place = me_pts * CORES + core

    def dev_plane(step):
        at = lax.rem(place + step, plane)
        return {"pts": at // CORES, "med": zed * CORES + lax.rem(at, CORES)}

    partners = [dev_z(step) for step in range(1, n_z)] + [dev_plane(step) for step in range(1, plane)]

    def points_copy(tile):
        part_of = pl.ds(pl.multiple_of(tile * TILE, TILE), TILE)
        return pltpu.make_async_copy(points_ref.at[part_of], pbuf.at[part_of], psem.at[tile])

    own_copy = pltpu.make_async_copy(mine_ref, recv.at[core, i_2, i_1, zed], msem)
    own_copy.start()
    for tile in range(tiles):
        points_copy(tile).start()
    barrier = pltpu.get_barrier_semaphore()
    for partner in partners:
        pl.semaphore_signal(barrier, inc=1, device_id=partner, device_id_type=pl.DeviceIdType.MESH)

    width = n_z * CAPACITY
    depth = points_ref.shape[1]
    ids = ids_ref[...]

    def offsets(which, j_2, j_1):
        at = lax.broadcasted_iota(jnp.int32, (width, 1), 0)
        z = at // CAPACITY
        slot = at - z * CAPACITY
        first = (pts_of(which, j_1, j_2) * group_med + z * CORES + which) * rows
        inside = jnp.logical_and(ids >= first, ids < first + rows)
        count = jnp.sum(jnp.where(inside, 1.0, 0.0), axis=1, keepdims=True)
        offs[which, j_2, j_1] = jnp.where(slot.astype(jnp.float32) < count, 0.0, -1e30)

    def offsets_at(at, carry):
        which = at // (n_1 * n_2)
        j_2 = lax.rem(at, n_1 * n_2) // n_1
        offsets(which, j_2, lax.rem(at, n_1))
        return carry

    lax.fori_loop(0, CORES * n_1 * n_2, offsets_at, 0)
    best[...] = jnp.full(best.shape, -1e30, jnp.float32)
    pl.semaphore_wait(barrier, len(partners))

    def send(src, j_2, j_1, z, sem, partner):
        return pltpu.make_async_remote_copy(
            src_ref=src,
            dst_ref=recv.at[core, j_2, j_1, z],
            send_sem=sem,
            recv_sem=rsem.at[core, j_2, j_1, z],
            device_id=partner,
            device_id_type=pl.DeviceIdType.MESH,
        )

    def send_z(step):
        return send(mine_ref, i_2, i_1, zed, zsem.at[step], dev_z(step))

    def send_1(z, step, src=None):
        src = recv.at[core, i_2, i_1, z] if src is None else src
        return send(src, i_2, i_1, z, fsem.at[z, step], dev_1(step))

    def send_2(j_1, z, step, src=None):
        src = recv.at[core, i_2, j_1, z] if src is None else src
        return send(src, i_2, j_1, z, ssem.at[j_1, z, step], dev_2(step))

    def send_b(j_2, j_1, z, src=None):
        src = recv.at[core, j_2, j_1, z] if src is None else src
        return send(src, j_2, j_1, z, bsem.at[j_2, j_1, z], sibling)

    def arrived(which, j_2, j_1, z):
        slot = recv.at[which, j_2, j_1, z]
        pltpu.make_async_copy(slot, slot, rsem.at[which, j_2, j_1, z]).wait()

    def z_at(step):
        return lax.rem(zed + step, n_z)

    def one_at(step):
        return lax.rem(i_1 + step, n_1)

    def two_at(step):
        return lax.rem(i_2 + step, n_2)

    for step in range(1, n_1):
        send_1(zed, step, mine_ref).start()
    for step in range(1, n_2):
        send_2(i_1, zed, step, mine_ref).start()
    for step in [1, n_z - 1] + list(range(2, n_z - 1)) if n_z > 2 else range(1, n_z):
        send_z(step).start()
    send_b(i_2, i_1, zed, mine_ref).start()

    def prepare(tile, carry):
        points_copy(tile).wait()

        def piece(step, carry):
            part_of = pl.ds(pl.multiple_of(tile * TILE + step * PIECE, PIECE), PIECE)
            total = jnp.zeros((8, PIECE), jnp.float32)
            for k in range(0, depth, 128):
                value = pbuf[part_of, k : k + 128].T
                high, low = split(value)
                pcat[k : k + 128, part_of] = high
                pcat[depth + k : depth + k + 128, part_of] = low
                pcat[2 * depth + k : 2 * depth + k + 128, part_of] = high
                total = total + jnp.sum((value * value).reshape(-1, 8, PIECE), axis=0)
            norm = jnp.sum(total, axis=0, keepdims=True)
            scale_ref[:, part_of] = lax.rsqrt(norm + EPS)
            return carry

        lax.fori_loop(0, TILE // PIECE, piece, 0)
        return carry

    lax.fori_loop(0, tiles, prepare, 0)
    own_copy.wait()

    z_order = [1, n_z - 1] + list(range(2, n_z - 1)) if n_z > 2 else list(range(1, n_z))
    for step in z_order:
        z = z_at(step)
        arrived(core, i_2, i_1, z)
        for hop in range(1, n_1):
            send_1(z, hop).start()
        for hop in range(1, n_2):
            send_2(i_1, z, hop).start()
        send_b(i_2, i_1, z).start()

    def load_chunk(which, j_2, j_1, base):
        def pair(step, carry):
            value = recv[which, j_2, j_1, pl.ds(step * 2, 2)].reshape(2 * CAPACITY, depth)
            high, low = split(value)
            part_of = pl.ds(pl.multiple_of(base + step * 2 * CAPACITY, 2 * CAPACITY), 2 * CAPACITY)
            ccat[part_of, 0:depth] = high
            ccat[part_of, depth : 2 * depth] = high
            ccat[part_of, 2 * depth : 3 * depth] = low
            return carry

        lax.fori_loop(0, n_z // 2, pair, 0)

    dims = (((1,), (0,)), ((), ()))

    def multiply(tile, mask):
        part_of = pl.ds(pl.multiple_of(tile * TILE, TILE), TILE)
        sims = lax.dot_general(ccat[...], pcat[:, part_of], dims, preferred_element_type=jnp.float32)
        sims = sims + mask()
        top = jnp.max(sims.reshape(-1, 8, TILE), axis=0)
        best[:, part_of] = jnp.maximum(best[:, part_of], top)

    def event_1(e):
        hop = e // n_z + 1
        z = z_at(lax.rem(e, n_z))
        j_1 = one_at(hop)
        arrived(core, i_2, j_1, z)
        for far in range(1, n_2):
            send_2(j_1, z, far).start()
        send_b(i_2, j_1, z).start()

    def event_2(one, e):
        hop = e // n_z + 1
        z = z_at(lax.rem(e, n_z))
        j_2 = two_at(hop)
        arrived(core, j_2, one_at(one), z)
        send_b(j_2, one_at(one), z).start()

    def chunk(e_2, e_1, event, events):
        for z in range(n_z):
            if swap:
                s_2, s_1 = lax.rem(o_2 + e_2, n_2), lax.rem(o_1 + e_1, n_1)
            else:
                s_2, s_1 = two_at(e_2), one_at(e_1)
            arrived(other, s_2, s_1, z)
        load_chunk(core, two_at(e_2), one_at(e_1), 0)
        load_chunk(other, s_2, s_1, width)

        def mask():
            return jnp.concatenate(
                [offs[core, two_at(e_2), one_at(e_1)], offs[other, s_2, s_1]], axis=0
            )

        def step(tile, carry):
            if events:
                @pl.when(tile < events)
                def _():
                    event(tile)
            multiply(tile, mask)
            return carry

        lax.fori_loop(0, tiles, step, 0)
        if events > tiles:
            def rest(e, carry):
                event(e)
                return carry

            lax.fori_loop(tiles, events, rest, 0)

    order = [(e_2, e_1) for e_2 in range(n_2) for e_1 in range(n_1)]
    for e_2, e_1 in order:
        if e_2 == 0 and e_1 == 0:
            chunk(0, 0, event_1, (n_1 - 1) * n_z)
        elif e_2 == 0:
            last = e_1 == n_1 - 1
            if last:
                chunk(0, e_1, functools.partial(event_2, 0), (n_2 - 1) * n_z)
            else:
                chunk(0, e_1, None, 0)
        elif e_2 == 1:
            if e_1 + 1 < n_1:
                chunk(1, e_1, functools.partial(event_2, e_1 + 1), (n_2 - 1) * n_z)
            else:
                chunk(1, e_1, None, 0)
        else:
            chunk(e_2, e_1, None, 0)

    cover = jnp.max(best[...], axis=0, keepdims=True) * scale_ref[...]
    cover_ref[...] = cover
    weights = weights_ref[...]
    lane = lax.broadcasted_iota(jnp.int32, (8, 128), 1)
    number = jnp.sum(weights * cover, axis=1, keepdims=True)
    weight = jnp.sum(weights, axis=1, keepdims=True)
    value = jnp.where(lane == 0, number, weight)

    stages = [(n_z, zed, dev_z), (plane, place, dev_plane)]
    copies = []
    for stage, (extent, index, partner_of) in enumerate(stages):
        if extent == 1:
            continue
        part[stage] = value
        for step in range(1, extent):
            copy = pltpu.make_async_remote_copy(
                src_ref=part.at[stage],
                dst_ref=tin.at[stage, index],
                send_sem=tsend.at[stage, step],
                recv_sem=trecv.at[stage, index],
                device_id=partner_of(step),
                device_id_type=pl.DeviceIdType.MESH,
            )
            copy.start()
            copies.append(copy)
        for step in range(1, extent):
            where = lax.rem(index + step, extent)
            slot = tin.at[stage, where]
            pltpu.make_async_copy(slot, slot, trecv.at[stage, where]).wait()
        tin[stage, index] = value
        value = tin[stage, 0]
        for at in range(1, extent):
            value = value + tin[stage, at]
    total_ref[...] = value[:, 0:1] / value[:, 1:2] + jnp.zeros((8, 128), jnp.float32)

    for step in range(1, n_z):
        send_z(step).wait_send()
    for z in range(n_z):
        for step in range(1, n_1):
            send_1(z, step).wait_send()
        for j_1 in range(n_1):
            for step in range(1, n_2):
                send_2(j_1, z, step).wait_send()
            for j_2 in range(n_2):
                send_b(j_2, j_1, z).wait_send()
    for copy in copies:
        copy.wait_send()


def finish_kernel(cover_ref, total_ref, out_ref, mean_ref):
    out_ref[...] = cover_ref[...]
    mean_ref[0, 0] = total_ref[0, 0]


def body(points, weights, medoid_ids):
    rows, width = points.shape
    group_pts = lax.axis_size("pts")
    group_med = lax.axis_size("med")
    n_z, n_a = group_med // CORES, 2
    n_1, n_2 = group_pts // n_a, n_a
    start = (lax.axis_index("pts") * group_med + lax.axis_index("med")) * rows
    smem = pl.BlockSpec(memory_space=pltpu.SMEM)
    vmem = pl.BlockSpec(memory_space=pltpu.VMEM)
    hbm = pl.BlockSpec(memory_space=pl.ANY)
    mine = pl.pallas_call(
        gather_kernel,
        out_shape=jax.ShapeDtypeStruct((CAPACITY, width), jnp.float32),
        in_specs=[smem, smem, hbm],
        out_specs=vmem,
        scratch_shapes=[
            pltpu.SMEM((CAPACITY + 1,), jnp.int32),
            pltpu.VMEM((CAPACITY, width), jnp.float32),
            pltpu.SemaphoreType.DMA((CAPACITY,)),
        ],
        name="gather_rows",
    )(start[None].astype(jnp.int32), medoid_ids, points)

    chunk = CORES * n_z * CAPACITY
    top = max(n_z, group_pts * CORES)
    dma = pltpu.SemaphoreType.DMA
    cover, total = pl.pallas_call(
        functools.partial(cover_kernel, group_pts, group_med),
        out_shape=[
            jax.ShapeDtypeStruct((1, rows), jnp.float32),
            jax.ShapeDtypeStruct((8, 128), jnp.float32),
        ],
        in_specs=[vmem, hbm, vmem, vmem],
        out_specs=[vmem, vmem],
        scratch_shapes=[
            pltpu.VMEM((CORES, n_2, n_1, n_z, CAPACITY, width), jnp.float32),
            pltpu.VMEM((rows, width), jnp.float32),
            pltpu.VMEM((3 * width, rows), jnp.bfloat16),
            pltpu.VMEM((chunk, 3 * width), jnp.bfloat16),
            pltpu.VMEM((CORES, n_2, n_1, n_z * CAPACITY, 1), jnp.float32),
            pltpu.VMEM((1, rows), jnp.float32),
            pltpu.VMEM((8, rows), jnp.float32),
            pltpu.VMEM((2, 8, 128), jnp.float32),
            pltpu.VMEM((2, top, 8, 128), jnp.float32),
            dma((rows // TILE,)),
            dma,
            dma((CORES, n_2, n_1, n_z)),
            dma((n_z,)),
            dma((n_z, n_1)),
            dma((n_1, n_z, n_2)),
            dma((n_2, n_1, n_z)),
            dma((2, top)),
            dma((2, top)),
        ],
        compiler_params=pltpu.CompilerParams(
            collective_id=0, has_side_effects=True, vmem_limit_bytes=60 * 1024 * 1024
        ),
        name="cover_all",
    )(mine, points, weights[None, :], medoid_ids[None, :])
    cover, total = pl.pallas_call(
        finish_kernel,
        out_shape=[
            jax.ShapeDtypeStruct((1, rows), jnp.float32),
            jax.ShapeDtypeStruct((1, 1), jnp.float32),
        ],
        in_specs=[vmem, vmem],
        out_specs=[vmem, smem],
        name="finish",
    )(cover, total)
    return cover.reshape(rows), total.reshape(())


def solution(mesh):
    return jax.shard_map(
        body,
        mesh=mesh,
        in_specs=(P(("pts", "med"), None), P(("pts", "med")), P()),
        out_specs=(P(("pts", "med")), P()),
        check_vma=False,
    )
```
